32 devices in a mesh: gx: 8 (over y, x, core), gy: 4 (over z).
Axes of the slice: x: 2, y: 2, z: 4, core: 2. Of those that a mesh axis runs over, the one named last changes fastest.
Arguments:
- ocean_heat_field: float32 [8, 192, 128, 128], P('gy', 'gx'), may hold values from -6 to 6
- patch_zone: int32 [192], replicated, may hold values from 0 to 31, as said below
- patch_position: int32 [192], replicated, may hold values from 0 to 11, as said below
- quarter_spins: int32 [192], replicated, may hold values from 0 to 3
- zone_patch_tally: int32 [32], P(('gx', 'gy')), may hold values from 0 to 12, as said below
Outputs:
- regional: float32 [8, 32, 12, 128, 128], P(None, ('gx', 'gy'))
The draws below stay inside these ranges and needn't reach their ends.
Inputs may be any that keep to these rules, and one draw needn't show every extreme that they name: In each aligned group of 24 blocks no more than 6 go to regions of one column patch_zone // 4, and each group has a column with exactly 6. A region receives at most 12 blocks and some region receives exactly 12. `patch_position`: the blocks of one region have distinct slots 0 to zone_patch_tally of that region minus 1, in increasing block order. zone_patch_tally[r] is the number of blocks j with patch_zone[j] = r.
All inputs are finite; a program needn't handle non-finite values.
Results may differ from the reference program's by a relative error of at most 0.00002.
Values sent between devices are 32-bit elements; how exact they have to be, the bound alone decides.
A program may use at most 128 MiB of HBM per device.

```python
import jax
import jax.numpy as jnp

PATCH_SIDE = 128
BLK_DEV = 24
INPUT_PATCHES = 192
EPOCH_TOTAL = 8
REGIONS = 32
MOST = 6
CAP = 12


def rank_within(labels, label_count):
    onehot = (labels[:, None] == jnp.arange(label_count, dtype=jnp.int32)[None, :]).astype(jnp.int32)
    running = jnp.cumsum(onehot, axis=0) - onehot
    return jnp.sum(running * onehot, axis=1).astype(jnp.int32)


def routing(key):
    column_count = INPUT_PATCHES // BLK_DEV
    row_count = REGIONS // column_count
    column_slots = column_count * MOST
    group_key = jax.random.fold_in(key, 101)
    order_key = jax.random.fold_in(key, 202)

    def group_columns(subkey):
        pick_key, score_key, shuffle_key = jax.random.split(subkey, 3)
        chosen = jax.random.randint(pick_key, (), 0, column_count, dtype=jnp.int32)
        slot_ids = jnp.arange(column_slots, dtype=jnp.int32)
        scores = jax.random.permutation(score_key, column_slots).astype(jnp.int32)
        scores = jnp.where(slot_ids // MOST == chosen, slot_ids % MOST - MOST, scores)
        ranked = jnp.argsort(scores, stable=True).astype(jnp.int32)
        return jax.random.permutation(shuffle_key, ranked[:BLK_DEV] // MOST)
    columns = jax.vmap(group_columns)(jax.random.split(group_key, column_count)).reshape(-1)

    def column_order(subkey):
        pick_key, score_key = jax.random.split(subkey)
        chosen = jax.random.randint(pick_key, (), 0, row_count, dtype=jnp.int32)
        slot_ids = jnp.arange(column_slots, dtype=jnp.int32)
        scores = jax.random.permutation(score_key, column_slots).astype(jnp.int32)
        scores = jnp.where(slot_ids // CAP == chosen, slot_ids % CAP - CAP, scores)
        return jnp.argsort(scores, stable=True).astype(jnp.int32)
    orders = jax.vmap(column_order)(jax.random.split(order_key, column_count))
    within = rank_within(columns, column_count)
    rows = orders[columns, within] // CAP
    regions = (columns * row_count + rows).astype(jnp.int32)
    slots = rank_within(regions, REGIONS)
    counts = jnp.sum((regions[:, None] == jnp.arange(REGIONS, dtype=jnp.int32)[None, :]).astype(jnp.int32), axis=0)
    return (regions, slots, counts.astype(jnp.int32))


def draw_patch_zone(key, part):
    return routing(key)[0]


def draw_patch_position(key, part):
    return routing(key)[1]


def draw_zone_patch_tally(key, part):
    return routing(key)[2]


def plant(array, key, smallest, largest):
    shape = array.shape
    index_at = [jax.random.randint(jax.random.fold_in(key, axis), (), 0, shape[axis]) for axis in range(len(shape))]
    array = array.at[tuple(index_at)].set(smallest)
    longest = shape.index(max(shape))
    index_at[longest] = (index_at[longest] + 1) % shape[longest]
    return array.at[tuple(index_at)].set(largest)


def level_of(rng, extent, pieces, low, high):
    def one(axis_at, blocks):
        heights = jax.random.uniform(jax.random.fold_in(jax.random.fold_in(rng, 6), axis_at), (blocks,), jnp.float32, low / len(pieces), high / len(pieces))
        return jnp.repeat(jnp.exp(heights), extent[axis_at] // blocks).reshape((-1,) + (1,) * (len(extent) - axis_at - 1))

    loudness = one(*pieces[0])
    for cut in pieces[1:]:
        loudness = loudness * one(*cut)
    return loudness


def noise(rng, dims, deviation, limit, cuts=(), kind=jnp.bfloat16):
    result = jax.random.normal(rng, dims, jnp.float32) * deviation
    if len(cuts) > 0:
        result = level_of(rng, dims, cuts, -0.22, 0.18) * result
    return jnp.clip(result, min=-limit, max=limit).astype(kind)


def setup_inputs(seed: int = 0) -> dict:
    streams_of = jax.random.split(jax.random.key(seed), 6)
    return {
        "ocean_heat_field": noise(streams_of[0], (EPOCH_TOTAL, INPUT_PATCHES, PATCH_SIDE, PATCH_SIDE), 1.0, 6.0, ((0, 4), (1, 8)), jnp.float32),
        "patch_zone": draw_patch_zone(jax.random.fold_in(streams_of[5], 71), 0),
        "patch_position": draw_patch_position(jax.random.fold_in(streams_of[5], 71), 0),
        "quarter_spins": plant(jax.random.randint(streams_of[3], (INPUT_PATCHES,), 0, 4), jax.random.fold_in(streams_of[3], 1), 0, 3).astype(jnp.int32),
        "zone_patch_tally": draw_zone_patch_tally(jax.random.fold_in(streams_of[5], 71), 0),
    }


def spin_patches(incoming_patches, turn_codes):
    first_turn = jnp.rot90(incoming_patches, 1, axes=(2, 3))
    half_turn = jnp.rot90(incoming_patches, 2, axes=(2, 3))
    last_turn = jnp.rot90(incoming_patches, 3, axes=(2, 3))
    shaped = turn_codes[None, :, None, None]
    return jnp.where(shaped == 0, incoming_patches, jnp.where(shaped == 1, first_turn, jnp.where(shaped == 2, half_turn, last_turn)))


def reference(ocean_heat_field, patch_zone, patch_position, quarter_spins, zone_patch_tally):
    spun_patches = spin_patches(ocean_heat_field, quarter_spins)
    centered = spun_patches - jnp.mean(spun_patches, axis=0, keepdims=True)
    arranged = jnp.zeros((EPOCH_TOTAL, REGIONS, CAP, PATCH_SIDE, PATCH_SIDE), jnp.float32)
    arranged = arranged.at[:, patch_zone, patch_position].set(centered)
    in_use = jnp.arange(CAP, dtype=jnp.int32)[None, :] < zone_patch_tally[:, None]
    return jnp.where(in_use[None, :, :, None, None], arranged, jnp.float32(0.0))
```

```python
import functools

import jax
import jax.numpy as jnp
from jax import lax
from jax.experimental import pallas as pl
from jax.experimental.pallas import tpu as pltpu
from jax.sharding import PartitionSpec as P

MESH = pl.DeviceIdType.MESH
CHUNKS = 4
STEP_BLOCKS = 4
CODE = 1024


def mirror_lanes(block):
    side = block.shape[1]
    lane = side - 1 - lax.broadcasted_iota(jnp.int32, block.shape, 1)
    return jnp.take_along_axis(block, lane, axis=1)


def prepare(dims, zone, slot, spins, field, turned, send_table, pick_table, first_tally, peaks, counts, fills):
    pairs, rows, per_group, per_pair, per_row = dims
    gx = lax.axis_index("gx")
    pair = gx // 2
    group = 2 * per_group
    step = pl.program_id(0)

    @pl.when(step == 0)
    def _():
        def clear(ref, size):
            def body(i, c):
                ref[i] = 0
                return c
            lax.fori_loop(0, size, body, 0)
        clear(send_table, pairs * per_pair)
        clear(pick_table, rows * per_row)
        clear(counts, 2 * pairs * rows)
        clear(fills, pairs * pairs)

        def tally(j, c):
            region = zone[j]
            counts[region] = counts[region] + 1
            return c
        lax.fori_loop(0, pairs * group, tally, 0)
        for r in range(rows):
            first_tally[r] = counts[2 * pair * rows + r]
        most_row = jnp.int32(0)
        for q in range(pairs):
            for r in range(rows):
                most_row = jnp.maximum(most_row, counts[2 * q * rows + r] + counts[(2 * q + 1) * rows + r])

        def place(j, c):
            region = zone[j]
            source = j // group
            target = region // (2 * rows)
            cell = source * pairs + target
            rank = fills[cell]
            fills[cell] = rank + 1

            @pl.when(source == pair)
            def _():
                ahead = lax.rem(target - pair + pairs, pairs)
                send_table[ahead * per_pair + rank] = j - source * group

            @pl.when(target == pair)
            def _():
                behind = lax.rem(pair - source + pairs, pairs)
                row = lax.rem(region, rows)
                second = lax.rem(region // rows, 2)
                at = slot[j] + second * counts[2 * pair * rows + row]
                pick_table[row * per_row + at] = behind * CODE + rank
            return c
        lax.fori_loop(0, pairs * group, place, 0)
        most_pair = jnp.int32(0)
        for q in range(pairs):
            for r in range(pairs):
                if q != r:
                    most_pair = jnp.maximum(most_pair, fills[q * pairs + r])
        peaks[0] = most_pair
        peaks[1] = most_row

    times, blocks, side, _ = field.shape
    halves, chunks, _, _, part, _ = turned.shape
    for b in range(blocks):
        code = spins[gx * per_group + step * blocks + b]
        for kind in range(4):
            @pl.when(code == kind)
            def _(kind=kind, b=b):
                for t in range(times):
                    block = field[t, b]
                    if kind == 1:
                        block = mirror_lanes(block).T
                    elif kind == 2:
                        block = mirror_lanes(mirror_lanes(block).T).T
                    elif kind == 3:
                        block = mirror_lanes(block.T)
                    turned[:, :, b, t] = block.reshape(halves, chunks, part, side)


def exchange(dims, send_table, pick_table, first_tally, turned, final, *scratch):
    pairs, rows, per_group, per_pair, wide, tall, cap = dims
    chunks = turned.shape[1]
    held, packed, landed, lifted, risen, given, kept = (
        scratch[i * chunks:(i + 1) * chunks] for i in range(7)
    )
    (own_sem, swap_send, swap_recv, pair_send, pair_recv, row_send, row_recv, give_send, give_recv, keep_sem) = scratch[7 * chunks:]
    gx = lax.axis_index("gx")
    z = lax.axis_index("gy")
    pair = gx // 2
    half = lax.rem(gx, 2)
    mate = (2 * pair + 1 - half, z)

    def across(o):
        return (2 * lax.rem(pair + o, pairs) + half, z)

    def along(o):
        return (gx, lax.rem(z + o, rows))

    barrier = pltpu.get_barrier_semaphore()
    friends = [mate] + [across(o) for o in range(1, pairs)] + [along(o) for o in range(1, rows)]
    for friend in friends:
        pl.semaphore_signal(barrier, inc=1, device_id=friend, device_id_type=MESH)
    own_copies = []
    for c in range(chunks):
        own = pltpu.make_async_copy(turned.at[half, c], held[c].at[pl.ds(half * per_group, per_group)], own_sem.at[c])
        own.start()
        own_copies.append(own)
    pl.semaphore_wait(barrier, len(friends))

    swaps = []
    for c in range(chunks):
        swap = pltpu.make_async_remote_copy(
            src_ref=turned.at[1 - half, c], dst_ref=held[c].at[pl.ds(half * per_group, per_group)],
            send_sem=swap_send.at[c], recv_sem=swap_recv.at[c], device_id=mate, device_id_type=MESH)
        swap.start()
        swaps.append(swap)

    pending = []
    pair_copies = []
    for c in range(chunks):
        own_copies[c].wait()
        swaps[c].wait_recv()
        sent = []
        for o in list(range(1, pairs)):
            def pack(k, carry, o=o, c=c):
                packed[c][o - 1, k] = held[c][send_table[o * per_pair + k]]
                return carry
            lax.fori_loop(0, wide, pack, 0, unroll=2)
            copy = pltpu.make_async_remote_copy(
                src_ref=packed[c].at[o - 1], dst_ref=landed[c].at[pl.ds(per_pair + (o - 1) * wide, wide)],
                send_sem=pair_send.at[c, o - 1], recv_sem=pair_recv.at[c, o - 1],
                device_id=across(o), device_id_type=MESH)
            copy.start()
            sent.append(copy)

        def stay(k, carry, c=c):
            landed[c][k] = held[c][send_table[k]]
            return carry
        lax.fori_loop(0, per_pair, stay, 0, unroll=2)
        pair_copies.append(sent)

    def source_of(code):
        behind = code // CODE
        rank = lax.rem(code, CODE)
        return rank + jnp.where(behind > 0, per_pair + (behind - 1) * wide, 0)

    row_copies = []
    for c in range(chunks):
        for copy in pair_copies[c]:
            copy.wait_recv()
        sent = []
        for o in list(range(rows - 1, 0, -1)) + [0]:
            row = lax.rem(z + o, rows)

            def lift(k, carry, o=o, c=c, row=row):
                tile = landed[c][source_of(pick_table[row * 2 * cap + k])]
                if o > 0:
                    lifted[c][o - 1, k] = tile
                else:
                    risen[c][0, k] = tile
                return carry
            lax.fori_loop(0, tall, lift, 0, unroll=2)
            if o > 0:
                copy = pltpu.make_async_remote_copy(
                    src_ref=lifted[c].at[o - 1], dst_ref=risen[c].at[o],
                    send_sem=row_send.at[c, o - 1], recv_sem=row_recv.at[c, o - 1],
                    device_id=along(o), device_id_type=MESH)
                copy.start()
                sent.append(copy)
        row_copies.append(sent)

    first = first_tally[z]
    gives = []
    for c in range(chunks):
        for copy in row_copies[c]:
            copy.wait_recv()

        def settle(s, carry, c=c):
            mine = jnp.minimum(s + half * first, tall - 1)
            other = jnp.minimum(s + (1 - half) * first, tall - 1)
            for o in range(rows):
                given[c][s, o] = risen[c][o, other]
                kept[c][s, o] = risen[c][o, mine]
            return carry
        lax.fori_loop(0, cap, settle, 0)
        give = pltpu.make_async_remote_copy(
            src_ref=given[c], dst_ref=final.at[half, c],
            send_sem=give_send.at[c], recv_sem=give_recv.at[c], device_id=mate, device_id_type=MESH)
        give.start()
        keep = pltpu.make_async_copy(kept[c], final.at[half, c], keep_sem.at[c])
        keep.start()
        gives.append((give, keep))
    for c in range(chunks):
        swaps[c].wait_send()
        for copy in pair_copies[c] + row_copies[c]:
            copy.wait_send()
        gives[c][0].wait()
        gives[c][1].wait()


def finish(rows, tally, final, regional):
    z = lax.axis_index("gy")
    slot = pl.program_id(0)
    halves, chunks, _, _, times, part, side = final.shape

    @pl.when(slot < tally[0])
    def _():
        for h in range(halves):
            for c in range(chunks):
                span = pl.ds((h * chunks + c) * part, part)
                tiles = [[final[h, c, 0, o, t] for t in range(times)] for o in range(rows)]
                total = sum(tile for row in tiles for tile in row)
                mean = total * jnp.float32(1.0 / (rows * times))
                for o in range(rows):
                    start = lax.rem(z - o + rows, rows) * times
                    for t in range(times):
                        regional[start + t, 0, 0, span, :] = tiles[o][t] - mean

    @pl.when(slot >= tally[0])
    def _():
        regional[...] = jnp.zeros_like(regional)


def levels(most, steps):
    return sorted({-(-most * s // 24) for s in steps})


def on_device(field, zone, slot, spins, tally):
    times, per_group, side, _ = field.shape
    columns = lax.axis_size("gx")
    rows = lax.axis_size("gy")
    pairs = columns // 2
    cap = 2 * per_group // rows
    per_pair = 4 * (2 * per_group // columns)
    per_row = 2 * cap
    halves, chunks = 2, CHUNKS
    part = side // (halves * chunks)
    smem = pl.BlockSpec(memory_space=pltpu.SMEM)
    anywhere = pl.BlockSpec(memory_space=pl.ANY)
    i32 = jnp.int32
    turned, send_table, pick_table, first_tally, peaks = pl.pallas_call(
        functools.partial(prepare, (pairs, rows, per_group, per_pair, per_row)),
        grid=(per_group // STEP_BLOCKS,),
        in_specs=[smem, smem, smem, pl.BlockSpec((times, STEP_BLOCKS, side, side), lambda i: (0, i, 0, 0))],
        out_specs=[
            pl.BlockSpec((halves, chunks, STEP_BLOCKS, times, part, side), lambda i: (0, 0, i, 0, 0, 0)),
            smem, smem, smem, smem,
        ],
        out_shape=[
            jax.ShapeDtypeStruct((halves, chunks, per_group, times, part, side), jnp.float32),
            jax.ShapeDtypeStruct((pairs * per_pair,), i32),
            jax.ShapeDtypeStruct((rows * per_row,), i32),
            jax.ShapeDtypeStruct((rows,), i32),
            jax.ShapeDtypeStruct((2,), i32),
        ],
        scratch_shapes=[pltpu.SMEM((columns * rows,), i32), pltpu.SMEM((pairs * pairs,), i32)],
        name="prepare",
    )(zone, slot, spins, field)

    tile = (times, part, side)

    def moved(wide, tall, tag):
        def vmem(*lead):
            return [pltpu.VMEM(lead + tile, jnp.float32)] * chunks
        dma = pltpu.SemaphoreType.DMA
        return lambda: pl.pallas_call(
            functools.partial(exchange, (pairs, rows, per_group, per_pair, wide, tall, cap)),
            in_specs=[smem, smem, smem, anywhere],
            out_specs=anywhere,
            out_shape=jax.ShapeDtypeStruct((halves, chunks, cap, rows) + tile, jnp.float32),
            scratch_shapes=[
                *vmem(2 * per_group),
                *vmem(pairs - 1, wide),
                *vmem(per_pair + (pairs - 1) * wide),
                *vmem(rows - 1, tall),
                *vmem(rows, tall),
                *vmem(cap, rows),
                *vmem(cap, rows),
                dma((chunks,)), dma((chunks,)), dma((chunks,)),
                dma((chunks, pairs - 1)), dma((chunks, pairs - 1)),
                dma((chunks, rows - 1)), dma((chunks, rows - 1)),
                dma((chunks,)), dma((chunks,)), dma((chunks,)),
            ],
            compiler_params=pltpu.CompilerParams(collective_id=tag, has_side_effects=True, vmem_limit_bytes=60 * 2**20),
            name=f"exchange_{tag}",
        )(send_table, pick_table, first_tally, turned)

    sizes = [(levels(per_pair, (20, 24))[0], level) for level in levels(per_row, (17, 19, 21))]
    sizes.append((per_pair, per_row))
    fits = [jnp.logical_and(peaks[0] <= wide, peaks[1] <= tall) for wide, tall in sizes[:-1]]
    choice = sum(jnp.logical_not(fit).astype(i32) for fit in fits)
    final = lax.switch(choice, [moved(wide, tall, tag) for tag, (wide, tall) in enumerate(sizes)])

    return pl.pallas_call(
        functools.partial(finish, rows),
        grid_spec=pltpu.PrefetchScalarGridSpec(
            num_scalar_prefetch=1,
            grid=(cap,),
            in_specs=[pl.BlockSpec(
                (halves, chunks, 1, rows) + tile,
                lambda s, count: (0, 0, jnp.maximum(jnp.minimum(s, count[0] - 1), 0), 0, 0, 0, 0))],
            out_specs=pl.BlockSpec((rows * times, 1, 1, side, side), lambda s, count: (0, 0, s, 0, 0)),
        ),
        out_shape=jax.ShapeDtypeStruct((rows * times, 1, cap, side, side), jnp.float32),
        name="finish",
    )(tally, final)


def solution(mesh):
    placed = (P("gy", "gx", None, None), P(), P(), P(), P(("gx", "gy")))
    return jax.shard_map(
        on_device,
        mesh=mesh,
        in_specs=placed,
        out_specs=P(None, ("gx", "gy"), None, None, None),
        check_vma=False,
    )
```

```python
import functools

import jax
import jax.numpy as jnp
from jax import lax
from jax.experimental import pallas as pl
from jax.experimental.pallas import tpu as pltpu
from jax.sharding import PartitionSpec as P

MESH = pl.DeviceIdType.MESH
CHUNKS = 8
STEP_BLOCKS = 4


def mirror_lanes(block):
    side = block.shape[1]
    lane = side - 1 - lax.broadcasted_iota(jnp.int32, block.shape, 1)
    return jnp.take_along_axis(block, lane, axis=1)


def prepare(dims, zone, slot, spins, field, turned, send_table, pick_table, tallies, peaks, counts, fills):
    pairs, rows, per_group, per_pair, cap = dims
    gx = lax.axis_index("gx")
    pair = gx // 2
    group = 2 * per_group
    local = 2 * rows
    step = pl.program_id(0)

    @pl.when(step == 0)
    def _():
        def clear(ref, size):
            def body(i, c):
                ref[i] = 0
                return c
            lax.fori_loop(0, size, body, 0, unroll=8)
        clear(send_table, pairs * per_pair + 1)
        clear(pick_table, local * cap + 1)
        clear(counts, pairs * local)
        clear(fills, pairs * pairs)

        for source in range(pairs):
            behind = lax.rem(pair - source + pairs, pairs) * per_pair

            def place(j, c, source=source, behind=behind):
                region = zone[source * group + j]
                counts[region] = counts[region] + 1
                target = region // local
                cell = source * pairs + target
                rank = fills[cell]
                fills[cell] = rank + 1
                ahead = lax.rem(target - source + pairs, pairs) * per_pair
                send_table[jnp.where(source == pair, ahead + rank, pairs * per_pair)] = j
                at = (region - target * local) * cap + slot[source * group + j]
                pick_table[jnp.where(target == pair, at, local * cap)] = behind + rank
                return c
            lax.fori_loop(0, group, place, 0, unroll=4)
        most_pair = jnp.int32(0)
        most_row = jnp.int32(0)
        most_half = jnp.int32(0)
        for q in range(pairs):
            for r in range(pairs):
                if q != r:
                    most_pair = jnp.maximum(most_pair, fills[q * pairs + r])
            pooled = [counts[q * local + r] + counts[q * local + rows + r] for r in range(rows)]
            for value in pooled:
                most_row = jnp.maximum(most_row, value)
            for side_rows in (pooled[:rows // 2], pooled[rows // 2:]):
                most_half = jnp.maximum(most_half, sum(side_rows))
        for r in range(local):
            tallies[r] = counts[pair * local + r]
        peaks[0] = most_pair
        peaks[1] = most_row
        peaks[2] = most_half

    times, blocks, side, _ = field.shape
    halves, chunks, _, _, part, _ = turned.shape
    for b in range(blocks):
        code = spins[gx * per_group + step * blocks + b]
        for kind in range(4):
            @pl.when(code == kind)
            def _(kind=kind, b=b):
                for t in range(times):
                    block = field[t, b]
                    if kind == 1:
                        block = mirror_lanes(block).T
                    elif kind == 2:
                        block = mirror_lanes(mirror_lanes(block).T).T
                    elif kind == 3:
                        block = mirror_lanes(block.T)
                    turned[:, :, b, t] = block.reshape(halves, chunks, part, side)


def origin_of(z, rows, k):
    if rows != 4:
        return lax.rem(z - k + rows, rows)
    low = z < 2
    return [z, z + 1 - 2 * lax.rem(z, 2), jnp.where(low, 2, 1), jnp.where(low, 3, 0)][k]


def exchange(dims, send_table, pick_table, tallies, turned, final, *scratch):
    pairs, rows, per_group, per_pair, wide, tall, far, cap = dims
    relay = rows == 4
    chunks = turned.shape[1]
    kinds = 10 if relay else 7
    groups = [scratch[i * chunks:(i + 1) * chunks] for i in range(kinds)]
    held, packed, landed, lifted, risen, given, kept = groups[:7]
    sems = list(scratch[kinds * chunks:])
    row_list = sems.pop(0)
    own_sem, swap_send, swap_recv, pair_send, pair_recv, row_send, row_recv, give_send, give_recv, keep_sem = sems[:10]
    gx = lax.axis_index("gx")
    z = lax.axis_index("gy")
    pair = gx // 2
    half = lax.rem(gx, 2)
    mate = (2 * pair + 1 - half, z)

    def across(o):
        return (2 * lax.rem(pair + o, pairs) + half, z)

    def along(o):
        return (gx, lax.rem(z + o, rows))

    barrier = pltpu.get_barrier_semaphore()
    friends = [mate] + [across(o) for o in range(1, pairs)] + [along(o) for o in range(1, rows)]
    for friend in friends:
        pl.semaphore_signal(barrier, inc=1, device_id=friend, device_id_type=MESH)
    own_copies = []
    for c in range(chunks):
        own = pltpu.make_async_copy(turned.at[half, c], held[c].at[pl.ds(half * per_group, per_group)], own_sem.at[c])
        own.start()
        own_copies.append(own)
    pl.semaphore_wait(barrier, len(friends))

    swaps = []
    for c in range(chunks):
        swap = pltpu.make_async_remote_copy(
            src_ref=turned.at[1 - half, c], dst_ref=held[c].at[pl.ds(half * per_group, per_group)],
            send_sem=swap_send.at[c], recv_sem=swap_recv.at[c], device_id=mate, device_id_type=MESH)
        swap.start()
        swaps.append(swap)

    unsent = []
    pair_copies = []
    for c in range(chunks):
        own_copies[c].wait()
        swaps[c].wait_recv()
        unsent.append(swaps[c])
        sent = []
        for o in range(1, pairs):
            def pack(k, carry, o=o, c=c):
                packed[c][o - 1, k] = held[c][send_table[o * per_pair + k]]
                return carry
            lax.fori_loop(0, wide, pack, 0, unroll=4)
            copy = pltpu.make_async_remote_copy(
                src_ref=packed[c].at[o - 1], dst_ref=landed[c].at[pl.ds(o * per_pair, wide)],
                send_sem=pair_send.at[c, o - 1], recv_sem=pair_recv.at[c, o - 1],
                device_id=across(o), device_id_type=MESH)
            copy.start()
            sent.append(copy)
        unsent.extend(sent)

        def stay(k, carry, c=c):
            landed[c][k] = held[c][send_table[k]]
            return carry
        lax.fori_loop(0, per_pair, stay, 0, unroll=4)
        pair_copies.append(sent)

    for r in range(rows):
        first = tallies[r]

        def compact(k, carry, r=r, first=first):
            at = jnp.minimum(jnp.where(k < first, r * cap + k, (rows + r) * cap + k - first), 2 * rows * cap - 1)
            row_list[r * tall + k] = pick_table[at]
            return carry
        lax.fori_loop(0, tall, compact, 0, unroll=4)

    gives = []

    def settle_all(c):
        first = tallies[z]

        def settle(s, carry, c=c):
            mine = jnp.minimum(s + half * first, tall - 1)
            other = jnp.minimum(s + (1 - half) * first, tall - 1)
            for o in range(rows):
                given[c][s, o] = risen[c][o, other]
                kept[c][s, o] = risen[c][o, mine]
            return carry
        lax.fori_loop(0, cap, settle, 0)
        give = pltpu.make_async_remote_copy(
            src_ref=given[c], dst_ref=final.at[half, c],
            send_sem=give_send.at[c], recv_sem=give_recv.at[c], device_id=mate, device_id_type=MESH)
        give.start()
        keep = pltpu.make_async_copy(kept[c], final.at[half, c], keep_sem.at[c])
        keep.start()
        gives.append((give, keep))

    if not relay:
        row_copies = []
        for c in range(chunks):
            for copy in pair_copies[c]:
                copy.wait_recv()
            sent = []
            for o in list(range(rows - 1, 0, -1)) + [0]:
                row = lax.rem(z + o, rows)

                def lift(k, carry, o=o, c=c, row=row):
                    tile = landed[c][row_list[row * tall + k]]
                    if o > 0:
                        lifted[c][o - 1, k] = tile
                    else:
                        risen[c][0, k] = tile
                    return carry
                lax.fori_loop(0, tall, lift, 0, unroll=4)
                if o > 0:
                    copy = pltpu.make_async_remote_copy(
                        src_ref=lifted[c].at[o - 1], dst_ref=risen[c].at[o],
                        send_sem=row_send.at[c, o - 1], recv_sem=row_recv.at[c, o - 1],
                        device_id=along(o), device_id_type=MESH)
                    copy.start()
                    sent.append(copy)
            row_copies.append(sent)
            unsent.extend(sent)
        for c in range(chunks):
            for copy in row_copies[c]:
                copy.wait_recv()
            settle_all(c)
    else:
        pooled, crossed, passed = groups[7:10]
        far_list, far_send, far_recv, pass_send, pass_recv = sems[10:]
        near, far_in, far_out = (origin_of(z, rows, k) for k in (1, 2, 3))
        inner = jnp.logical_or(z == 1, z == 2)
        outer = jnp.logical_not(inner)
        role = jnp.where(inner, 0, 1)
        lead = tallies[far_in] + tallies[rows + far_in]
        skip = tallies[z] + tallies[rows + z]

        def gather_far(k, carry):
            at = jnp.where(k < lead, far_in * tall + k, far_out * tall + k - lead)
            far_list[k] = row_list[jnp.minimum(at, rows * tall - 1)]
            return carry
        lax.fori_loop(0, far, gather_far, 0, unroll=4)

        near_copies = {}

        def far_copy(c, place):
            return pltpu.make_async_remote_copy(
                src_ref=pooled[c], dst_ref=crossed[c].at[place],
                send_sem=far_send.at[c], recv_sem=far_recv.at[c, place],
                device_id=(gx, far_in), device_id_type=MESH)

        def pass_copy(c, place):
            return pltpu.make_async_remote_copy(
                src_ref=passed[c].at[place], dst_ref=risen[c].at[2 + place],
                send_sem=pass_send.at[c, place], recv_sem=pass_recv.at[c, place],
                device_id=(gx, near), device_id_type=MESH)

        def send_rows(c):
            for copy in pair_copies[c]:
                copy.wait_recv()

            def pool(k, carry):
                pooled[c][k] = landed[c][far_list[k]]
                return carry
            lax.fori_loop(0, far, pool, 0, unroll=4)
            copy = far_copy(c, role)
            copy.start()
            unsent.append(copy)

            def lift(k, carry):
                lifted[c][k] = landed[c][row_list[near * tall + k]]
                return carry
            lax.fori_loop(0, tall, lift, 0, unroll=4)
            copy = pltpu.make_async_remote_copy(
                src_ref=lifted[c], dst_ref=risen[c].at[1],
                send_sem=row_send.at[c], recv_sem=row_recv.at[c],
                device_id=(gx, near), device_id_type=MESH)
            copy.start()
            unsent.append(copy)
            near_copies[c] = copy

            def own(k, carry):
                risen[c][0, k] = landed[c][row_list[z * tall + k]]
                return carry
            lax.fori_loop(0, tall, own, 0, unroll=4)

        def hand_on(c):
            @pl.when(inner)
            def _():
                for place in range(2):
                    far_copy(c, place).wait_recv()
                for place in range(2):
                    def onward(k, carry, place=place):
                        passed[c][place, k] = crossed[c][place, jnp.minimum(skip + k, far - 1)]
                        return carry
                    lax.fori_loop(0, tall, onward, 0, unroll=4)
                    pass_copy(c, place).start()

                    def land(k, carry, place=place):
                        risen[c][2 + place, k] = crossed[c][place, k]
                        return carry
                    lax.fori_loop(0, tall, land, 0, unroll=4)

        def close(c):
            near_copies[c].wait_recv()

            @pl.when(outer)
            def _():
                for place in range(2):
                    pass_copy(c, place).wait_recv()
            settle_all(c)

        pace = far / wide
        events = []
        for c in range(chunks):
            events.append((c + 1.0, 0, c, send_rows))
            events.append((1.0 + pace * (c + 1), 1, c, hand_on))
            events.append((1.0 + pace * (c + 2), 2, c, close))
        for _, _, c, act in sorted(events, key=lambda e: e[:3]):
            act(c)

        @pl.when(inner)
        def _():
            for c in range(chunks):
                for place in range(2):
                    pass_copy(c, place).wait_send()

    for copy in unsent:
        copy.wait_send()
    for give, keep in gives:
        give.wait()
        keep.wait()


def finish(rows, tally, final, regional):
    z = lax.axis_index("gy")
    slot = pl.program_id(0)
    halves, chunks, _, _, times, part, side = final.shape

    @pl.when(slot < tally[0])
    def _():
        for h in range(halves):
            for c in range(chunks):
                span = pl.ds((h * chunks + c) * part, part)
                tiles = [[final[h, c, 0, o, t] for t in range(times)] for o in range(rows)]
                total = sum(tile for row in tiles for tile in row)
                mean = total * jnp.float32(1.0 / (rows * times))
                for o in range(rows):
                    start = origin_of(z, rows, o) * times
                    for t in range(times):
                        regional[start + t, 0, 0, span, :] = tiles[o][t] - mean

    @pl.when(slot >= tally[0])
    def _():
        regional[...] = jnp.zeros_like(regional)


def levels(most, steps):
    return sorted({-(-most * s // 48) for s in steps})


def on_device(field, zone, slot, spins, tally):
    times, per_group, side, _ = field.shape
    columns = lax.axis_size("gx")
    rows = lax.axis_size("gy")
    pairs = columns // 2
    cap = 2 * per_group // rows
    per_pair = 4 * (2 * per_group // columns)
    per_row = 2 * cap
    halves, chunks = 2, CHUNKS
    part = side // (halves * chunks)
    smem = pl.BlockSpec(memory_space=pltpu.SMEM)
    anywhere = pl.BlockSpec(memory_space=pl.ANY)
    i32 = jnp.int32
    turned, send_table, pick_table, tallies, peaks = pl.pallas_call(
        functools.partial(prepare, (pairs, rows, per_group, per_pair, cap)),
        grid=(per_group // STEP_BLOCKS,),
        in_specs=[smem, smem, smem, pl.BlockSpec((times, STEP_BLOCKS, side, side), lambda i: (0, i, 0, 0))],
        out_specs=[
            pl.BlockSpec((halves, chunks, STEP_BLOCKS, times, part, side), lambda i: (0, 0, i, 0, 0, 0)),
            smem, smem, smem, smem,
        ],
        out_shape=[
            jax.ShapeDtypeStruct((halves, chunks, per_group, times, part, side), jnp.float32),
            jax.ShapeDtypeStruct((pairs * per_pair + 1,), i32),
            jax.ShapeDtypeStruct((per_row * rows + 1,), i32),
            jax.ShapeDtypeStruct((2 * rows,), i32),
            jax.ShapeDtypeStruct((3,), i32),
        ],
        scratch_shapes=[pltpu.SMEM((columns * rows,), i32), pltpu.SMEM((pairs * pairs,), i32)],
        name="prepare",
    )(zone, slot, spins, field)

    tile = (times, part, side)

    relay = rows == 4

    def moved(wide, tall, far, tag):
        def vmem(*lead):
            return [pltpu.VMEM(lead + tile, jnp.float32)] * chunks
        dma = pltpu.SemaphoreType.DMA
        along = (chunks,) if relay else (chunks, rows - 1)
        buffers = [
            *vmem(2 * per_group),
            *vmem(pairs - 1, wide),
            *vmem(pairs * per_pair),
            *(vmem(tall) if relay else vmem(rows - 1, tall)),
            *vmem(rows, tall),
            *vmem(cap, rows),
            *vmem(cap, rows),
            *(vmem(far) + vmem(2, far) + vmem(2, tall) if relay else []),
            pltpu.SMEM((rows * tall,), i32),
            dma((chunks,)), dma((chunks,)), dma((chunks,)),
            dma((chunks, pairs - 1)), dma((chunks, pairs - 1)),
            dma(along), dma(along),
            dma((chunks,)), dma((chunks,)), dma((chunks,)),
        ]
        if relay:
            buffers += [pltpu.SMEM((far,), i32), dma((chunks,)), dma((chunks, 2)), dma((chunks, 2)), dma((chunks, 2))]
        return lambda: pl.pallas_call(
            functools.partial(exchange, (pairs, rows, per_group, per_pair, wide, tall, far, cap)),
            in_specs=[smem, smem, smem, anywhere],
            out_specs=anywhere,
            out_shape=jax.ShapeDtypeStruct((halves, chunks, cap, rows) + tile, jnp.float32),
            scratch_shapes=buffers,
            compiler_params=pltpu.CompilerParams(collective_id=tag, has_side_effects=True, vmem_limit_bytes=60 * 2**20),
            name=f"exchange_{tag}",
        )(send_table, pick_table, tallies, turned)

    narrow = levels(per_pair, (40,))[0]
    if relay:
        sizes = [(narrow, per_row, far) for far in levels(2 * per_row, (30, 32, 34, 36, 38))]
    else:
        sizes = [(narrow, tall, 2 * per_row) for tall in levels(per_row, (36, 42))]
    sizes.append((per_pair, per_row, 2 * per_row))

    def fitting(wide, tall, far):
        low = jnp.logical_and(peaks[0] <= wide, peaks[1] <= tall)
        return jnp.logical_and(low, peaks[2] <= far) if relay else low
    choice = sum(jnp.logical_not(fitting(*size)).astype(i32) for size in sizes[:-1])
    final = lax.switch(choice, [moved(*size, tag) for tag, size in enumerate(sizes)])

    return pl.pallas_call(
        functools.partial(finish, rows),
        grid_spec=pltpu.PrefetchScalarGridSpec(
            num_scalar_prefetch=1,
            grid=(cap,),
            in_specs=[pl.BlockSpec(
                (halves, chunks, 1, rows) + tile,
                lambda s, count: (0, 0, jnp.maximum(jnp.minimum(s, count[0] - 1), 0), 0, 0, 0, 0))],
            out_specs=pl.BlockSpec((rows * times, 1, 1, side, side), lambda s, count: (0, 0, s, 0, 0)),
        ),
        out_shape=jax.ShapeDtypeStruct((rows * times, 1, cap, side, side), jnp.float32),
        name="finish",
    )(tally, final)


def solution(mesh):
    placed = (P("gy", "gx", None, None), P(), P(), P(), P(("gx", "gy")))
    return jax.shard_map(
        on_device,
        mesh=mesh,
        in_specs=placed,
        out_specs=P(None, ("gx", "gy"), None, None, None),
        check_vma=False,
    )
```

```python
import functools

import jax
import jax.numpy as jnp
from jax import lax
from jax.experimental import pallas as pl
from jax.experimental.pallas import tpu as pltpu
from jax.sharding import PartitionSpec as P

MESH = pl.DeviceIdType.MESH
PART = 8
STEP_BLOCKS = 4


def chunk_units(times, side):
    units = [(r, t) for r in range(side // (2 * PART)) for t in range(times)]
    small = 2 * (times // 2 + times % 2)
    cuts = list(range(0, small + 1, max(times // 2, 1)))
    cuts += list(range(small + times, len(units) - small + 1, times))
    cuts += list(range(len(units) - small + max(times // 2, 1), len(units) + 1, max(times // 2, 1)))
    return [units[a:b] for a, b in zip(cuts[:-1], cuts[1:])]


def mirror_lanes(block):
    side = block.shape[1]
    lane = side - 1 - lax.broadcasted_iota(jnp.int32, block.shape, 1)
    return jnp.take_along_axis(block, lane, axis=1)


def prepare(dims, zone, slot, spins, field, *refs):
    pairs, rows, per_group, per_pair, cap, chunks = dims
    turned = refs[:len(chunks)]
    send_table, pick_table, tallies, peaks, counts, fills = refs[len(chunks):]
    gx = lax.axis_index("gx")
    pair = gx // 2
    group = 2 * per_group
    local = 2 * rows
    step = pl.program_id(0)

    @pl.when(step == 0)
    def _():
        def clear(ref, size):
            def body(i, c):
                ref[i] = 0
                return c
            lax.fori_loop(0, size, body, 0, unroll=8)
        clear(send_table, pairs * per_pair + 1)
        clear(pick_table, local * cap + 1)
        clear(counts, pairs * local)
        clear(fills, pairs * pairs)

        for source in range(pairs):
            behind = lax.rem(pair - source + pairs, pairs) * per_pair

            def place(j, c, source=source, behind=behind):
                region = zone[source * group + j]
                counts[region] = counts[region] + 1
                target = region // local
                cell = source * pairs + target
                rank = fills[cell]
                fills[cell] = rank + 1
                ahead = lax.rem(target - source + pairs, pairs) * per_pair
                send_table[jnp.where(source == pair, ahead + rank, pairs * per_pair)] = j
                at = (region - target * local) * cap + slot[source * group + j]
                pick_table[jnp.where(target == pair, at, local * cap)] = behind + rank
                return c
            lax.fori_loop(0, group, place, 0, unroll=4)
        most_pair = jnp.int32(0)
        most_row = jnp.int32(0)
        most_half = jnp.int32(0)
        for q in range(pairs):
            for r in range(pairs):
                if q != r:
                    most_pair = jnp.maximum(most_pair, fills[q * pairs + r])
            pooled = [counts[q * local + r] + counts[q * local + rows + r] for r in range(rows)]
            for value in pooled:
                most_row = jnp.maximum(most_row, value)
            for side_rows in (pooled[:rows // 2], pooled[rows // 2:]):
                most_half = jnp.maximum(most_half, sum(side_rows))
        for r in range(local):
            tallies[r] = counts[pair * local + r]
        peaks[0] = most_pair
        peaks[1] = most_row
        peaks[2] = most_half

    times, blocks, side, _ = field.shape
    for b in range(blocks):
        code = spins[gx * per_group + step * blocks + b]
        for kind in range(4):
            @pl.when(code == kind)
            def _(kind=kind, b=b):
                for t in range(times):
                    block = field[t, b]
                    if kind == 1:
                        block = mirror_lanes(block).T
                    elif kind == 2:
                        block = mirror_lanes(mirror_lanes(block).T).T
                    elif kind == 3:
                        block = mirror_lanes(block.T)
                    for c, chunk in enumerate(chunks):
                        for i, (r, at) in enumerate(chunk):
                            if at == t:
                                for h in range(2):
                                    top = h * (side // 2) + r * PART
                                    turned[c][h, b, i] = block[top:top + PART]


def origin_of(z, rows, k):
    if rows != 4:
        return lax.rem(z - k + rows, rows)
    low = z < 2
    return [z, z + 1 - 2 * lax.rem(z, 2), jnp.where(low, 2, 1), jnp.where(low, 3, 0)][k]


def exchange(dims, send_table, pick_table, tallies, *refs):
    pairs, rows, per_group, per_pair, wide, tall, far, cap, starts = dims
    relay = rows == 4
    chunks = len(starts)
    turned, final, scratch = refs[:chunks], refs[chunks:2 * chunks], refs[2 * chunks:]
    kinds = 10 if relay else 7
    groups = [scratch[i * chunks:(i + 1) * chunks] for i in range(kinds)]
    held, packed, landed, lifted, risen, given, kept = groups[:7]
    sems = list(scratch[kinds * chunks:])
    row_list = sems.pop(0)
    own_sem, swap_send, swap_recv, pair_send, pair_recv, row_send, row_recv, give_send, give_recv, keep_sem = sems[:10]
    gx = lax.axis_index("gx")
    z = lax.axis_index("gy")
    pair = gx // 2
    half = lax.rem(gx, 2)
    mate = (2 * pair + 1 - half, z)

    def across(o):
        return (2 * lax.rem(pair + o, pairs) + half, z)

    def along(o):
        return (gx, lax.rem(z + o, rows))

    barrier = pltpu.get_barrier_semaphore()
    friends = [mate] + [across(o) for o in range(1, pairs)] + [along(o) for o in range(1, rows)]
    for friend in friends:
        pl.semaphore_signal(barrier, inc=1, device_id=friend, device_id_type=MESH)
    own_copies = []
    for c in range(chunks):
        own = pltpu.make_async_copy(turned[c].at[half], held[c].at[pl.ds(half * per_group, per_group)], own_sem.at[c])
        own.start()
        own_copies.append(own)
    pl.semaphore_wait(barrier, len(friends))

    swaps = []
    for c in range(chunks):
        swap = pltpu.make_async_remote_copy(
            src_ref=turned[c].at[1 - half], dst_ref=held[c].at[pl.ds(half * per_group, per_group)],
            send_sem=swap_send.at[c], recv_sem=swap_recv.at[c], device_id=mate, device_id_type=MESH)
        swap.start()
        swaps.append(swap)

    unsent = []
    pair_copies = []
    for c in range(chunks):
        own_copies[c].wait()
        swaps[c].wait_recv()
        unsent.append(swaps[c])
        sent = []
        for o in range(1, pairs):
            def pack(k, carry, o=o, c=c):
                packed[c][o - 1, k] = held[c][send_table[o * per_pair + k]]
                return carry
            lax.fori_loop(0, wide, pack, 0, unroll=4)
            copy = pltpu.make_async_remote_copy(
                src_ref=packed[c].at[o - 1], dst_ref=landed[c].at[pl.ds(o * per_pair, wide)],
                send_sem=pair_send.at[c, o - 1], recv_sem=pair_recv.at[c, o - 1],
                device_id=across(o), device_id_type=MESH)
            copy.start()
            sent.append(copy)
        unsent.extend(sent)

        def stay(k, carry, c=c):
            landed[c][k] = held[c][send_table[k]]
            return carry
        lax.fori_loop(0, per_pair, stay, 0, unroll=4)
        pair_copies.append(sent)

    for r in range(rows):
        first = tallies[r]

        def compact(k, carry, r=r, first=first):
            at = jnp.minimum(jnp.where(k < first, r * cap + k, (rows + r) * cap + k - first), 2 * rows * cap - 1)
            row_list[r * tall + k] = pick_table[at]
            return carry
        lax.fori_loop(0, tall, compact, 0, unroll=4)

    gives = []

    def settle_all(c):
        first = tallies[z]

        def settle(s, carry, c=c):
            mine = jnp.minimum(s + half * first, tall - 1)
            other = jnp.minimum(s + (1 - half) * first, tall - 1)
            for o in range(rows):
                given[c][s, o] = risen[c][o, other]
                kept[c][s, o] = risen[c][o, mine]
            return carry
        lax.fori_loop(0, cap, settle, 0)
        give = pltpu.make_async_remote_copy(
            src_ref=given[c], dst_ref=final[c].at[half],
            send_sem=give_send.at[c], recv_sem=give_recv.at[c], device_id=mate, device_id_type=MESH)
        give.start()
        keep = pltpu.make_async_copy(kept[c], final[c].at[half], keep_sem.at[c])
        keep.start()
        gives.append((give, keep))

    if not relay:
        row_copies = []
        for c in range(chunks):
            for copy in pair_copies[c]:
                copy.wait_recv()
            sent = []
            for o in list(range(rows - 1, 0, -1)) + [0]:
                row = lax.rem(z + o, rows)

                def lift(k, carry, o=o, c=c, row=row):
                    tile = landed[c][row_list[row * tall + k]]
                    if o > 0:
                        lifted[c][o - 1, k] = tile
                    else:
                        risen[c][0, k] = tile
                    return carry
                lax.fori_loop(0, tall, lift, 0, unroll=4)
                if o > 0:
                    copy = pltpu.make_async_remote_copy(
                        src_ref=lifted[c].at[o - 1], dst_ref=risen[c].at[o],
                        send_sem=row_send.at[c, o - 1], recv_sem=row_recv.at[c, o - 1],
                        device_id=along(o), device_id_type=MESH)
                    copy.start()
                    sent.append(copy)
            row_copies.append(sent)
            unsent.extend(sent)
        for c in range(chunks):
            for copy in row_copies[c]:
                copy.wait_recv()
            settle_all(c)
    else:
        pooled, crossed, passed = groups[7:10]
        far_list, far_send, far_recv, pass_send, pass_recv = sems[10:]
        near, far_in, far_out = (origin_of(z, rows, k) for k in (1, 2, 3))
        inner = jnp.logical_or(z == 1, z == 2)
        outer = jnp.logical_not(inner)
        role = jnp.where(inner, 0, 1)
        lead = tallies[far_in] + tallies[rows + far_in]
        skip = tallies[z] + tallies[rows + z]

        def gather_far(k, carry):
            at = jnp.where(k < lead, far_in * tall + k, far_out * tall + k - lead)
            far_list[k] = row_list[jnp.minimum(at, rows * tall - 1)]
            return carry
        lax.fori_loop(0, far, gather_far, 0, unroll=4)

        near_copies = {}

        def far_copy(c, place):
            return pltpu.make_async_remote_copy(
                src_ref=pooled[c], dst_ref=crossed[c].at[place],
                send_sem=far_send.at[c], recv_sem=far_recv.at[c, place],
                device_id=(gx, far_in), device_id_type=MESH)

        def pass_copy(c, place):
            return pltpu.make_async_remote_copy(
                src_ref=passed[c].at[place], dst_ref=risen[c].at[2 + place],
                send_sem=pass_send.at[c, place], recv_sem=pass_recv.at[c, place],
                device_id=(gx, near), device_id_type=MESH)

        def send_rows(c):
            for copy in pair_copies[c]:
                copy.wait_recv()

            def pool(k, carry):
                pooled[c][k] = landed[c][far_list[k]]
                return carry
            lax.fori_loop(0, far, pool, 0, unroll=4)
            copy = far_copy(c, role)
            copy.start()
            unsent.append(copy)

            def lift(k, carry):
                lifted[c][k] = landed[c][row_list[near * tall + k]]
                return carry
            lax.fori_loop(0, tall, lift, 0, unroll=4)
            copy = pltpu.make_async_remote_copy(
                src_ref=lifted[c], dst_ref=risen[c].at[1],
                send_sem=row_send.at[c], recv_sem=row_recv.at[c],
                device_id=(gx, near), device_id_type=MESH)
            copy.start()
            unsent.append(copy)
            near_copies[c] = copy

            def own(k, carry):
                risen[c][0, k] = landed[c][row_list[z * tall + k]]
                return carry
            lax.fori_loop(0, tall, own, 0, unroll=4)

        def hand_on(c):
            @pl.when(inner)
            def _():
                for place in range(2):
                    far_copy(c, place).wait_recv()
                for place in range(2):
                    def onward(k, carry, place=place):
                        passed[c][place, k] = crossed[c][place, jnp.minimum(skip + k, far - 1)]
                        return carry
                    lax.fori_loop(0, tall, onward, 0, unroll=4)
                    pass_copy(c, place).start()

                    def land(k, carry, place=place):
                        risen[c][2 + place, k] = crossed[c][place, k]
                        return carry
                    lax.fori_loop(0, tall, land, 0, unroll=4)

        def close(c):
            near_copies[c].wait_recv()

            @pl.when(outer)
            def _():
                for place in range(2):
                    pass_copy(c, place).wait_recv()
            settle_all(c)

        pace = far / wide
        events = []
        for c in range(chunks):
            begin, end = starts[c]
            events.append((float(end), 0, c, send_rows))
            events.append((starts[0][1] + pace * end, 1, c, hand_on))
            events.append((starts[0][1] + pace * (2 * end - begin), 2, c, close))
        for _, _, c, act in sorted(events, key=lambda e: (e[0], e[1], e[2])):
            act(c)

        @pl.when(inner)
        def _():
            for c in range(chunks):
                for place in range(2):
                    pass_copy(c, place).wait_send()

    for copy in unsent:
        copy.wait_send()
    for give, keep in gives:
        give.wait()
        keep.wait()


def finish(rows, chunks, tally, *refs):
    final, regional = refs[:-1], refs[-1]
    z = lax.axis_index("gy")
    slot = pl.program_id(0)
    side = regional.shape[3]
    times = regional.shape[0] // rows
    place = {unit: (c, i) for c, chunk in enumerate(chunks) for i, unit in enumerate(chunk)}

    @pl.when(slot < tally[0])
    def _():
        for h in range(2):
            for r in range(side // (2 * PART)):
                span = pl.ds(h * (side // 2) + r * PART, PART)
                tiles = {}
                for t in range(times):
                    c, i = place[(r, t)]
                    for o in range(rows):
                        tiles[o, t] = final[c][h, 0, o, i]
                mean = sum(tiles.values()) * jnp.float32(1.0 / (rows * times))
                for o in range(rows):
                    start = origin_of(z, rows, o) * times
                    for t in range(times):
                        regional[start + t, 0, 0, span, :] = tiles[o, t] - mean

    @pl.when(slot >= tally[0])
    def _():
        regional[...] = jnp.zeros_like(regional)


def levels(most, steps):
    return sorted({-(-most * s // 48) for s in steps})


def on_device(field, zone, slot, spins, tally):
    times, per_group, side, _ = field.shape
    columns = lax.axis_size("gx")
    rows = lax.axis_size("gy")
    pairs = columns // 2
    cap = 2 * per_group // rows
    per_pair = 4 * (2 * per_group // columns)
    per_row = 2 * cap
    chunks = chunk_units(times, side)
    tiles = [(len(chunk), PART, side) for chunk in chunks]
    ends = [sum(len(chunk) for chunk in chunks[:c + 1]) for c in range(len(chunks))]
    starts = tuple((end - tile[0], end) for end, tile in zip(ends, tiles))
    smem = pl.BlockSpec(memory_space=pltpu.SMEM)
    anywhere = pl.BlockSpec(memory_space=pl.ANY)
    i32 = jnp.int32
    *turned, send_table, pick_table, tallies, peaks = pl.pallas_call(
        functools.partial(prepare, (pairs, rows, per_group, per_pair, cap, chunks)),
        grid=(per_group // STEP_BLOCKS,),
        in_specs=[smem, smem, smem, pl.BlockSpec((times, STEP_BLOCKS, side, side), lambda i: (0, i, 0, 0))],
        out_specs=[
            *[pl.BlockSpec((2, STEP_BLOCKS) + tile, lambda i: (0, i, 0, 0, 0)) for tile in tiles],
            smem, smem, smem, smem,
        ],
        out_shape=[
            *[jax.ShapeDtypeStruct((2, per_group) + tile, jnp.float32) for tile in tiles],
            jax.ShapeDtypeStruct((pairs * per_pair + 1,), i32),
            jax.ShapeDtypeStruct((per_row * rows + 1,), i32),
            jax.ShapeDtypeStruct((2 * rows,), i32),
            jax.ShapeDtypeStruct((3,), i32),
        ],
        scratch_shapes=[pltpu.SMEM((columns * rows,), i32), pltpu.SMEM((pairs * pairs,), i32)],
        name="prepare",
    )(zone, slot, spins, field)

    relay = rows == 4

    def moved(wide, tall, far, tag):
        def vmem(*lead):
            return [pltpu.VMEM(lead + tile, jnp.float32) for tile in tiles]
        dma = pltpu.SemaphoreType.DMA
        count = len(chunks)
        along = (count,) if relay else (count, rows - 1)
        buffers = [
            *vmem(2 * per_group),
            *vmem(pairs - 1, wide),
            *vmem(pairs * per_pair),
            *(vmem(tall) if relay else vmem(rows - 1, tall)),
            *vmem(rows, tall),
            *vmem(cap, rows),
            *vmem(cap, rows),
            *(vmem(far) + vmem(2, far) + vmem(2, tall) if relay else []),
            pltpu.SMEM((rows * tall,), i32),
            dma((count,)), dma((count,)), dma((count,)),
            dma((count, pairs - 1)), dma((count, pairs - 1)),
            dma(along), dma(along),
            dma((count,)), dma((count,)), dma((count,)),
        ]
        if relay:
            buffers += [pltpu.SMEM((far,), i32), dma((count,)), dma((count, 2)), dma((count, 2)), dma((count, 2))]
        return lambda: pl.pallas_call(
            functools.partial(exchange, (pairs, rows, per_group, per_pair, wide, tall, far, cap, starts)),
            in_specs=[smem, smem, smem] + [anywhere] * count,
            out_specs=[anywhere] * count,
            out_shape=[jax.ShapeDtypeStruct((2, cap, rows) + tile, jnp.float32) for tile in tiles],
            scratch_shapes=buffers,
            compiler_params=pltpu.CompilerParams(collective_id=tag, has_side_effects=True, vmem_limit_bytes=60 * 2**20),
            name=f"exchange_{tag}",
        )(send_table, pick_table, tallies, *turned)

    narrow = levels(per_pair, (40,))[0]
    if relay:
        sizes = [(narrow, per_row, far) for far in levels(2 * per_row, (31, 33, 35, 37))]
    else:
        sizes = [(narrow, tall, 2 * per_row) for tall in levels(per_row, (36, 42))]
    sizes.append((per_pair, per_row, 2 * per_row))

    def fitting(wide, tall, far):
        low = jnp.logical_and(peaks[0] <= wide, peaks[1] <= tall)
        return jnp.logical_and(low, peaks[2] <= far) if relay else low
    choice = sum(jnp.logical_not(fitting(*size)).astype(i32) for size in sizes[:-1])
    final = lax.switch(choice, [moved(*size, tag) for tag, size in enumerate(sizes)])

    return pl.pallas_call(
        functools.partial(finish, rows, chunks),
        grid_spec=pltpu.PrefetchScalarGridSpec(
            num_scalar_prefetch=1,
            grid=(cap,),
            in_specs=[pl.BlockSpec(
                (2, 1, rows) + tile,
                lambda s, count: (0, jnp.maximum(jnp.minimum(s, count[0] - 1), 0), 0, 0, 0, 0)) for tile in tiles],
            out_specs=pl.BlockSpec((rows * times, 1, 1, side, side), lambda s, count: (0, 0, s, 0, 0)),
        ),
        out_shape=jax.ShapeDtypeStruct((rows * times, 1, cap, side, side), jnp.float32),
        name="finish",
    )(tally, *final)


def solution(mesh):
    placed = (P("gy", "gx", None, None), P(), P(), P(), P(("gx", "gy")))
    return jax.shard_map(
        on_device,
        mesh=mesh,
        in_specs=placed,
        out_specs=P(None, ("gx", "gy"), None, None, None),
        check_vma=False,
    )
```

```python
import functools

import jax
import jax.numpy as jnp
from jax import lax
from jax.experimental import pallas as pl
from jax.experimental.pallas import tpu as pltpu
from jax.sharding import PartitionSpec as P

MESH = pl.DeviceIdType.MESH
PART = 8
STEP_BLOCKS = 4


def chunk_units(times, side):
    units = [(r, t) for r in range(side // (2 * PART)) for t in range(times)]
    small = 2 * (times // 2 + times % 2)
    cuts = list(range(0, small + 1, max(times // 2, 1)))
    cuts += list(range(small + times, len(units) - small + 1, times))
    cuts += list(range(len(units) - small + max(times // 2, 1), len(units) + 1, max(times // 2, 1)))
    return [units[a:b] for a, b in zip(cuts[:-1], cuts[1:])]


def mirror_lanes(block):
    side = block.shape[1]
    lane = side - 1 - lax.broadcasted_iota(jnp.int32, block.shape, 1)
    return jnp.take_along_axis(block, lane, axis=1)


def prepare(dims, zone, slot, spins, field, *refs):
    pairs, rows, per_group, per_pair, cap, chunks, sizes = dims
    turned = refs[:len(chunks)]
    send_table, pick_table, tallies, choice, counts, fills = refs[len(chunks):]
    gx = lax.axis_index("gx")
    pair = gx // 2
    group = 2 * per_group
    local = 2 * rows
    step = pl.program_id(0)

    @pl.when(step == 0)
    def _():
        def clear(ref, size):
            def body(i, c):
                ref[i] = 0
                return c
            lax.fori_loop(0, size, body, 0, unroll=8)
        clear(send_table, pairs * per_pair + 1)
        clear(pick_table, local * cap + 1)
        clear(counts, pairs * local)
        clear(fills, pairs * pairs)

        for source in range(pairs):
            behind = lax.rem(pair - source + pairs, pairs) * per_pair

            def place(j, c, source=source, behind=behind):
                region = zone[source * group + j]
                counts[region] = counts[region] + 1
                target = region // local
                cell = source * pairs + target
                rank = fills[cell]
                fills[cell] = rank + 1
                ahead = lax.rem(target - source + pairs, pairs) * per_pair
                send_table[jnp.where(source == pair, ahead + rank, pairs * per_pair)] = j
                at = (region - target * local) * cap + slot[source * group + j]
                pick_table[jnp.where(target == pair, at, local * cap)] = behind + rank
                return c
            lax.fori_loop(0, group, place, 0, unroll=4)
        most_pair = jnp.int32(0)
        most_row = jnp.int32(0)
        most_half = jnp.int32(0)
        most_end = jnp.int32(0)
        for q in range(pairs):
            for r in range(pairs):
                if q != r:
                    most_pair = jnp.maximum(most_pair, fills[q * pairs + r])
            pooled = [counts[q * local + r] + counts[q * local + rows + r] for r in range(rows)]
            for value in pooled:
                most_row = jnp.maximum(most_row, value)
            most_end = jnp.maximum(most_end, jnp.maximum(pooled[0], pooled[-1]))
            for side_rows in (pooled[:rows // 2], pooled[rows // 2:]):
                most_half = jnp.maximum(most_half, sum(side_rows))
        for r in range(local):
            tallies[r] = counts[pair * local + r]
        chosen = jnp.int32(len(sizes) - 1)
        for at in range(len(sizes) - 2, -1, -1):
            wide, tall, far, end = sizes[at]
            fits = jnp.logical_and(most_pair <= wide, most_row <= tall)
            if rows == 4:
                fits = jnp.logical_and(fits, jnp.logical_and(most_half <= far, most_end <= end))
            chosen = jnp.where(fits, at, chosen)
        choice[0] = chosen

    times, blocks, side, _ = field.shape
    for b in range(blocks):
        code = spins[gx * per_group + step * blocks + b]
        for kind in range(4):
            @pl.when(code == kind)
            def _(kind=kind, b=b):
                for t in range(times):
                    block = field[t, b]
                    if kind == 1:
                        block = mirror_lanes(block).T
                    elif kind == 2:
                        block = mirror_lanes(mirror_lanes(block).T).T
                    elif kind == 3:
                        block = mirror_lanes(block.T)
                    for c, chunk in enumerate(chunks):
                        for i, (r, at) in enumerate(chunk):
                            if at == t:
                                for h in range(2):
                                    top = h * (side // 2) + r * PART
                                    turned[c][h, b, i] = block[top:top + PART]


def origin_of(z, rows, k):
    if rows != 4:
        return lax.rem(z - k + rows, rows)
    low = z < 2
    return [z, z + 1 - 2 * lax.rem(z, 2), jnp.where(low, 2, 1), jnp.where(low, 3, 0)][k]


def exchange(dims, send_table, pick_table, tallies, *refs):
    pairs, rows, per_group, per_pair, wide, tall, far, end, cap, starts = dims
    relay = rows == 4
    chunks = len(starts)
    turned, final, scratch = refs[:chunks], refs[chunks:2 * chunks], refs[2 * chunks:]
    kinds = 10 if relay else 7
    groups = [scratch[i * chunks:(i + 1) * chunks] for i in range(kinds)]
    held, packed, landed, lifted, risen, given, kept = groups[:7]
    sems = list(scratch[kinds * chunks:])
    row_list = sems.pop(0)
    own_sem, swap_send, swap_recv, pair_send, pair_recv, row_send, row_recv, give_send, give_recv, keep_sem = sems[:10]
    gx = lax.axis_index("gx")
    z = lax.axis_index("gy")
    pair = gx // 2
    half = lax.rem(gx, 2)
    mate = (2 * pair + 1 - half, z)

    def across(o):
        return (2 * lax.rem(pair + o, pairs) + half, z)

    def along(o):
        return (gx, lax.rem(z + o, rows))

    barrier = pltpu.get_barrier_semaphore()
    friends = [mate] + [across(o) for o in range(1, pairs)] + [along(o) for o in range(1, rows)]
    for friend in friends:
        pl.semaphore_signal(barrier, inc=1, device_id=friend, device_id_type=MESH)
    own_copies = []
    for c in range(chunks):
        own = pltpu.make_async_copy(turned[c].at[half], held[c].at[pl.ds(half * per_group, per_group)], own_sem.at[c])
        own.start()
        own_copies.append(own)
    pl.semaphore_wait(barrier, len(friends))

    swaps = []
    for c in range(chunks):
        swap = pltpu.make_async_remote_copy(
            src_ref=turned[c].at[1 - half], dst_ref=held[c].at[pl.ds(half * per_group, per_group)],
            send_sem=swap_send.at[c], recv_sem=swap_recv.at[c], device_id=mate, device_id_type=MESH)
        swap.start()
        swaps.append(swap)

    unsent = []
    pair_copies = []
    for c in range(chunks):
        own_copies[c].wait()
        swaps[c].wait_recv()
        unsent.append(swaps[c])
        sent = []
        for o in range(1, pairs):
            def pack(k, carry, o=o, c=c):
                packed[c][o - 1, k] = held[c][send_table[o * per_pair + k]]
                return carry
            lax.fori_loop(0, wide, pack, 0, unroll=4)
            copy = pltpu.make_async_remote_copy(
                src_ref=packed[c].at[o - 1], dst_ref=landed[c].at[pl.ds(o * per_pair, wide)],
                send_sem=pair_send.at[c, o - 1], recv_sem=pair_recv.at[c, o - 1],
                device_id=across(o), device_id_type=MESH)
            copy.start()
            sent.append(copy)
        unsent.extend(sent)

        def stay(k, carry, c=c):
            landed[c][k] = held[c][send_table[k]]
            return carry
        lax.fori_loop(0, per_pair, stay, 0, unroll=4)
        pair_copies.append(sent)

    for r in range(rows):
        first = tallies[r]

        def compact(k, carry, r=r, first=first):
            at = jnp.minimum(jnp.where(k < first, r * cap + k, (rows + r) * cap + k - first), 2 * rows * cap - 1)
            row_list[r * tall + k] = pick_table[at]
            return carry
        lax.fori_loop(0, tall, compact, 0, unroll=4)

    gives = []

    def settle_all(c):
        first = tallies[z]

        def settle(s, carry, c=c):
            mine = jnp.minimum(s + half * first, tall - 1)
            other = jnp.minimum(s + (1 - half) * first, tall - 1)
            for o in range(rows):
                given[c][s, o] = risen[c][o, other]
                kept[c][s, o] = risen[c][o, mine]
            return carry
        lax.fori_loop(0, cap, settle, 0)
        give = pltpu.make_async_remote_copy(
            src_ref=given[c], dst_ref=final[c].at[half],
            send_sem=give_send.at[c], recv_sem=give_recv.at[c], device_id=mate, device_id_type=MESH)
        give.start()
        keep = pltpu.make_async_copy(kept[c], final[c].at[half], keep_sem.at[c])
        keep.start()
        gives.append((give, keep))

    if not relay:
        row_copies = []
        for c in range(chunks):
            for copy in pair_copies[c]:
                copy.wait_recv()
            sent = []
            for o in list(range(rows - 1, 0, -1)) + [0]:
                row = lax.rem(z + o, rows)

                def lift(k, carry, o=o, c=c, row=row):
                    tile = landed[c][row_list[row * tall + k]]
                    if o > 0:
                        lifted[c][o - 1, k] = tile
                    else:
                        risen[c][0, k] = tile
                    return carry
                lax.fori_loop(0, tall, lift, 0, unroll=4)
                if o > 0:
                    copy = pltpu.make_async_remote_copy(
                        src_ref=lifted[c].at[o - 1], dst_ref=risen[c].at[o],
                        send_sem=row_send.at[c, o - 1], recv_sem=row_recv.at[c, o - 1],
                        device_id=along(o), device_id_type=MESH)
                    copy.start()
                    sent.append(copy)
            row_copies.append(sent)
            unsent.extend(sent)
        for c in range(chunks):
            for copy in row_copies[c]:
                copy.wait_recv()
            settle_all(c)
    else:
        pooled, crossed, passed = groups[7:10]
        far_list, far_send, far_recv, pass_send, pass_recv = sems[10:]
        near, far_in, far_out = (origin_of(z, rows, k) for k in (1, 2, 3))
        inner = jnp.logical_or(z == 1, z == 2)
        outer = jnp.logical_not(inner)
        role = jnp.where(inner, 0, 1)
        lead = tallies[far_in] + tallies[rows + far_in]
        skip = tallies[z] + tallies[rows + z]

        def gather_far(k, carry):
            at = jnp.where(k < lead, far_in * tall + k, far_out * tall + k - lead)
            far_list[k] = row_list[jnp.minimum(at, rows * tall - 1)]
            return carry
        lax.fori_loop(0, far, gather_far, 0, unroll=4)

        near_copies = {}

        def far_copy(c, place):
            return pltpu.make_async_remote_copy(
                src_ref=pooled[c], dst_ref=crossed[c].at[place],
                send_sem=far_send.at[c], recv_sem=far_recv.at[c, place],
                device_id=(gx, far_in), device_id_type=MESH)

        def pass_copy(c, place):
            return pltpu.make_async_remote_copy(
                src_ref=passed[c].at[place], dst_ref=risen[c].at[2 + place, pl.ds(0, end)],
                send_sem=pass_send.at[c, place], recv_sem=pass_recv.at[c, place],
                device_id=(gx, near), device_id_type=MESH)

        def send_rows(c):
            for copy in pair_copies[c]:
                copy.wait_recv()

            def pool(k, carry):
                pooled[c][k] = landed[c][far_list[k]]
                return carry
            lax.fori_loop(0, far, pool, 0, unroll=4)
            copy = far_copy(c, role)
            copy.start()
            unsent.append(copy)

            def lift(k, carry):
                lifted[c][k] = landed[c][row_list[near * tall + k]]
                return carry
            lax.fori_loop(0, tall, lift, 0, unroll=4)
            copy = pltpu.make_async_remote_copy(
                src_ref=lifted[c], dst_ref=risen[c].at[1],
                send_sem=row_send.at[c], recv_sem=row_recv.at[c],
                device_id=(gx, near), device_id_type=MESH)
            copy.start()
            unsent.append(copy)
            near_copies[c] = copy

            def own(k, carry):
                risen[c][0, k] = landed[c][row_list[z * tall + k]]
                return carry
            lax.fori_loop(0, tall, own, 0, unroll=4)

        def hand_on(c):
            @pl.when(inner)
            def _():
                for place in range(2):
                    far_copy(c, place).wait_recv()
                for place in range(2):
                    def onward(k, carry, place=place):
                        passed[c][place, k] = crossed[c][place, jnp.minimum(skip + k, far - 1)]
                        return carry
                    lax.fori_loop(0, end, onward, 0, unroll=4)
                    pass_copy(c, place).start()

                    def land(k, carry, place=place):
                        risen[c][2 + place, k] = crossed[c][place, k]
                        return carry
                    lax.fori_loop(0, tall, land, 0, unroll=4)

        def close(c):
            near_copies[c].wait_recv()

            @pl.when(outer)
            def _():
                for place in range(2):
                    pass_copy(c, place).wait_recv()
            settle_all(c)

        pace = far / wide
        events = []
        for c in range(chunks):
            begin, close_at = starts[c]
            events.append((float(close_at), 0, c, send_rows))
            events.append((starts[0][1] + pace * close_at, 1, c, hand_on))
            events.append((starts[0][1] + pace * (2 * close_at - begin), 2, c, close))
        for _, _, c, act in sorted(events, key=lambda e: (e[0], e[1], e[2])):
            act(c)

        @pl.when(inner)
        def _():
            for c in range(chunks):
                for place in range(2):
                    pass_copy(c, place).wait_send()

    for copy in unsent:
        copy.wait_send()
    for give, keep in gives:
        give.wait()
        keep.wait()


def finish(rows, chunks, tally, *refs):
    final, regional = refs[:-1], refs[-1]
    z = lax.axis_index("gy")
    slot = pl.program_id(0)
    side = regional.shape[3]
    times = regional.shape[0] // rows
    place = {unit: (c, i) for c, chunk in enumerate(chunks) for i, unit in enumerate(chunk)}

    @pl.when(slot < tally[0])
    def _():
        for h in range(2):
            for r in range(side // (2 * PART)):
                span = pl.ds(h * (side // 2) + r * PART, PART)
                tiles = {}
                for t in range(times):
                    c, i = place[(r, t)]
                    for o in range(rows):
                        tiles[o, t] = final[c][h, 0, o, i]
                mean = sum(tiles.values()) * jnp.float32(1.0 / (rows * times))
                for o in range(rows):
                    start = origin_of(z, rows, o) * times
                    for t in range(times):
                        regional[start + t, 0, 0, span, :] = tiles[o, t] - mean

    @pl.when(slot >= tally[0])
    def _():
        regional[...] = jnp.zeros_like(regional)


def levels(most, steps):
    return sorted({-(-most * s // 48) for s in steps})


def on_device(field, zone, slot, spins, tally):
    times, per_group, side, _ = field.shape
    columns = lax.axis_size("gx")
    rows = lax.axis_size("gy")
    pairs = columns // 2
    cap = 2 * per_group // rows
    per_pair = 4 * (2 * per_group // columns)
    per_row = 2 * cap
    chunks = chunk_units(times, side)
    tiles = [(len(chunk), PART, side) for chunk in chunks]
    ends = [sum(len(chunk) for chunk in chunks[:c + 1]) for c in range(len(chunks))]
    starts = tuple((end - tile[0], end) for end, tile in zip(ends, tiles))
    smem = pl.BlockSpec(memory_space=pltpu.SMEM)
    anywhere = pl.BlockSpec(memory_space=pl.ANY)
    i32 = jnp.int32
    relay = rows == 4
    narrow = levels(per_pair, (40,))[0]
    if relay:
        ends = levels(per_row, (40, 48))
        sizes = [(narrow, per_row, far, end) for far in levels(2 * per_row, (32, 34, 36)) for end in ends]
    else:
        sizes = [(narrow, tall, 2 * per_row, tall) for tall in levels(per_row, (36, 42))]
    sizes.append((per_pair, per_row, 2 * per_row, per_row))
    *turned, send_table, pick_table, tallies, choice = pl.pallas_call(
        functools.partial(prepare, (pairs, rows, per_group, per_pair, cap, chunks, sizes)),
        grid=(per_group // STEP_BLOCKS,),
        in_specs=[smem, smem, smem, pl.BlockSpec((times, STEP_BLOCKS, side, side), lambda i: (0, i, 0, 0))],
        out_specs=[
            *[pl.BlockSpec((2, STEP_BLOCKS) + tile, lambda i: (0, i, 0, 0, 0)) for tile in tiles],
            smem, smem, smem, smem,
        ],
        out_shape=[
            *[jax.ShapeDtypeStruct((2, per_group) + tile, jnp.float32) for tile in tiles],
            jax.ShapeDtypeStruct((pairs * per_pair + 1,), i32),
            jax.ShapeDtypeStruct((per_row * rows + 1,), i32),
            jax.ShapeDtypeStruct((2 * rows,), i32),
            jax.ShapeDtypeStruct((1,), i32),
        ],
        scratch_shapes=[pltpu.SMEM((columns * rows,), i32), pltpu.SMEM((pairs * pairs,), i32)],
        name="prepare",
    )(zone, slot, spins, field)

    def moved(wide, tall, far, end, tag):
        def vmem(*lead):
            return [pltpu.VMEM(lead + tile, jnp.float32) for tile in tiles]
        dma = pltpu.SemaphoreType.DMA
        count = len(chunks)
        along = (count,) if relay else (count, rows - 1)
        buffers = [
            *vmem(2 * per_group),
            *vmem(pairs - 1, wide),
            *vmem(pairs * per_pair),
            *(vmem(tall) if relay else vmem(rows - 1, tall)),
            *vmem(rows, tall),
            *vmem(cap, rows),
            *vmem(cap, rows),
            *(vmem(far) + vmem(2, far) + vmem(2, end) if relay else []),
            pltpu.SMEM((rows * tall,), i32),
            dma((count,)), dma((count,)), dma((count,)),
            dma((count, pairs - 1)), dma((count, pairs - 1)),
            dma(along), dma(along),
            dma((count,)), dma((count,)), dma((count,)),
        ]
        if relay:
            buffers += [pltpu.SMEM((far,), i32), dma((count,)), dma((count, 2)), dma((count, 2)), dma((count, 2))]
        return lambda: pl.pallas_call(
            functools.partial(exchange, (pairs, rows, per_group, per_pair, wide, tall, far, end, cap, starts)),
            in_specs=[smem, smem, smem] + [anywhere] * count,
            out_specs=[anywhere] * count,
            out_shape=[jax.ShapeDtypeStruct((2, cap, rows) + tile, jnp.float32) for tile in tiles],
            scratch_shapes=buffers,
            compiler_params=pltpu.CompilerParams(collective_id=tag, has_side_effects=True, vmem_limit_bytes=60 * 2**20),
            name=f"exchange_{tag}",
        )(send_table, pick_table, tallies, *turned)

    final = lax.switch(choice[0], [moved(*size, tag) for tag, size in enumerate(sizes)])

    return pl.pallas_call(
        functools.partial(finish, rows, chunks),
        grid_spec=pltpu.PrefetchScalarGridSpec(
            num_scalar_prefetch=1,
            grid=(cap,),
            in_specs=[pl.BlockSpec(
                (2, 1, rows) + tile,
                lambda s, count: (0, jnp.maximum(jnp.minimum(s, count[0] - 1), 0), 0, 0, 0, 0)) for tile in tiles],
            out_specs=pl.BlockSpec((rows * times, 1, 1, side, side), lambda s, count: (0, 0, s, 0, 0)),
        ),
        out_shape=jax.ShapeDtypeStruct((rows * times, 1, cap, side, side), jnp.float32),
        name="finish",
    )(tally, *final)


def solution(mesh):
    placed = (P("gy", "gx", None, None), P(), P(), P(), P(("gx", "gy")))
    return jax.shard_map(
        on_device,
        mesh=mesh,
        in_specs=placed,
        out_specs=P(None, ("gx", "gy"), None, None, None),
        check_vma=False,
    )
```

```python
import functools

import jax
import jax.numpy as jnp
from jax import lax
from jax.experimental import pallas as pl
from jax.experimental.pallas import tpu as pltpu
from jax.sharding import PartitionSpec as P

MESH = pl.DeviceIdType.MESH
PART = 8
STEP_BLOCKS = 4


def chunk_units(times, side):
    units = [(r, t) for r in range(side // (2 * PART)) for t in range(times)]
    small = 2 * (times // 2 + times % 2)
    cuts = list(range(0, small + 1, max(times // 2, 1)))
    cuts += list(range(small + times, len(units) - small + 1, times))
    cuts += list(range(len(units) - small + max(times // 2, 1), len(units) + 1, max(times // 2, 1)))
    return [units[a:b] for a, b in zip(cuts[:-1], cuts[1:])]


def mirror_lanes(block):
    side = block.shape[1]
    lane = side - 1 - lax.broadcasted_iota(jnp.int32, block.shape, 1)
    return jnp.take_along_axis(block, lane, axis=1)


def prepare(dims, zone, slot, spins, field, *refs):
    pairs, rows, per_group, per_pair, cap, chunks, sizes = dims
    turned = refs[:len(chunks)]
    send_table, pick_table, tallies, choice, counts, fills = refs[len(chunks):]
    gx = lax.axis_index("gx")
    pair = gx // 2
    group = 2 * per_group
    local = 2 * rows
    step = pl.program_id(0)

    @pl.when(step == 0)
    def _():
        def clear(ref, size):
            def body(i, c):
                ref[i] = 0
                return c
            lax.fori_loop(0, size, body, 0, unroll=8)
        clear(send_table, pairs * per_pair + 1)
        clear(pick_table, local * cap + 1)
        clear(counts, pairs * local)
        clear(fills, pairs * pairs)

        for source in range(pairs):
            behind = lax.rem(pair - source + pairs, pairs) * per_pair

            def place(j, c, source=source, behind=behind):
                region = zone[source * group + j]
                counts[region] = counts[region] + 1
                target = region // local
                cell = source * pairs + target
                rank = fills[cell]
                fills[cell] = rank + 1
                ahead = lax.rem(target - source + pairs, pairs) * per_pair
                send_table[jnp.where(source == pair, ahead + rank, pairs * per_pair)] = j
                at = (region - target * local) * cap + slot[source * group + j]
                pick_table[jnp.where(target == pair, at, local * cap)] = behind + rank
                return c
            lax.fori_loop(0, group, place, 0, unroll=4)
        most_pair = jnp.int32(0)
        most_row = jnp.int32(0)
        most_half = jnp.int32(0)
        most_end = jnp.int32(0)
        for q in range(pairs):
            for r in range(pairs):
                if q != r:
                    most_pair = jnp.maximum(most_pair, fills[q * pairs + r])
            pooled = [counts[q * local + r] + counts[q * local + rows + r] for r in range(rows)]
            for value in pooled:
                most_row = jnp.maximum(most_row, value)
            most_end = jnp.maximum(most_end, jnp.maximum(pooled[0], pooled[-1]))
            for side_rows in (pooled[:rows // 2], pooled[rows // 2:]):
                most_half = jnp.maximum(most_half, sum(side_rows))
        for r in range(local):
            tallies[r] = counts[pair * local + r]
        chosen = jnp.int32(len(sizes) - 1)
        for at in range(len(sizes) - 2, -1, -1):
            wide, tall, far, end = sizes[at]
            fits = jnp.logical_and(most_pair <= wide, most_row <= tall)
            if rows == 4:
                fits = jnp.logical_and(fits, jnp.logical_and(most_half <= far, most_end <= end))
            chosen = jnp.where(fits, at, chosen)
        choice[0] = chosen

    times, blocks, side, _ = field.shape
    for b in range(blocks):
        code = spins[gx * per_group + step * blocks + b]
        for kind in range(4):
            @pl.when(code == kind)
            def _(kind=kind, b=b):
                for t in range(times):
                    block = field[t, b]
                    if kind == 1:
                        block = mirror_lanes(block).T
                    elif kind == 2:
                        block = mirror_lanes(mirror_lanes(block).T).T
                    elif kind == 3:
                        block = mirror_lanes(block.T)
                    for c, chunk in enumerate(chunks):
                        for i, (r, at) in enumerate(chunk):
                            if at == t:
                                for h in range(2):
                                    top = h * (side // 2) + r * PART
                                    turned[c][h, b, i] = block[top:top + PART]


def origin_of(z, rows, k):
    if rows != 4:
        return lax.rem(z - k + rows, rows)
    low = z < 2
    return [z, z + 1 - 2 * lax.rem(z, 2), jnp.where(low, 2, 1), jnp.where(low, 3, 0)][k]


def exchange(dims, send_table, pick_table, tallies, *refs):
    pairs, rows, per_group, per_pair, wide, tall, far, end, cap, starts = dims
    relay = rows == 4
    chunks = len(starts)
    turned, final, scratch = refs[:chunks], refs[chunks:2 * chunks], refs[2 * chunks:]
    kinds = 10 if relay else 7
    groups = [scratch[i * chunks:(i + 1) * chunks] for i in range(kinds)]
    held, packed, landed, lifted, risen, given, kept = groups[:7]
    sems = list(scratch[kinds * chunks:])
    row_list = sems.pop(0)
    own_sem, swap_send, swap_recv, pair_send, pair_recv, row_send, row_recv, give_send, give_recv, keep_sem = sems[:10]
    gx = lax.axis_index("gx")
    z = lax.axis_index("gy")
    pair = gx // 2
    half = lax.rem(gx, 2)
    mate = (2 * pair + 1 - half, z)

    def across(o):
        return (2 * lax.rem(pair + o, pairs) + half, z)

    def along(o):
        return (gx, lax.rem(z + o, rows))

    barrier = pltpu.get_barrier_semaphore()
    friends = [mate] + [across(o) for o in range(1, pairs)] + [along(o) for o in range(1, rows)]
    for friend in friends:
        pl.semaphore_signal(barrier, inc=1, device_id=friend, device_id_type=MESH)
    own_copies = []
    for c in range(chunks):
        own = pltpu.make_async_copy(turned[c].at[half], held[c].at[pl.ds(half * per_group, per_group)], own_sem.at[c])
        own.start()
        own_copies.append(own)
    pl.semaphore_wait(barrier, len(friends))

    swaps = []
    for c in range(chunks):
        swap = pltpu.make_async_remote_copy(
            src_ref=turned[c].at[1 - half], dst_ref=held[c].at[pl.ds(half * per_group, per_group)],
            send_sem=swap_send.at[c], recv_sem=swap_recv.at[c], device_id=mate, device_id_type=MESH)
        swap.start()
        swaps.append(swap)

    unsent = []
    pair_copies = {}

    def pack_chunk(c):
        own_copies[c].wait()
        swaps[c].wait_recv()
        unsent.append(swaps[c])
        sent = []
        for o in range(1, pairs):
            def pack(k, carry, o=o):
                packed[c][o - 1, k] = held[c][send_table[o * per_pair + k]]
                return carry
            lax.fori_loop(0, wide, pack, 0, unroll=4)
            copy = pltpu.make_async_remote_copy(
                src_ref=packed[c].at[o - 1], dst_ref=landed[c].at[pl.ds(o * per_pair, wide)],
                send_sem=pair_send.at[c, o - 1], recv_sem=pair_recv.at[c, o - 1],
                device_id=across(o), device_id_type=MESH)
            copy.start()
            sent.append(copy)
        unsent.extend(sent)

        def stay(k, carry):
            landed[c][k] = held[c][send_table[k]]
            return carry
        lax.fori_loop(0, per_pair, stay, 0, unroll=4)
        pair_copies[c] = sent

    ahead = 3
    early = [c for c in range(chunks) if not relay or starts[c][0] < ahead]
    for c in early:
        pack_chunk(c)

    for r in range(rows):
        first = tallies[r]

        def compact(k, carry, r=r, first=first):
            at = jnp.minimum(jnp.where(k < first, r * cap + k, (rows + r) * cap + k - first), 2 * rows * cap - 1)
            row_list[r * tall + k] = pick_table[at]
            return carry
        lax.fori_loop(0, tall, compact, 0, unroll=4)

    gives = []

    def settle_all(c):
        first = tallies[z]

        def settle(s, carry, c=c):
            mine = jnp.minimum(s + half * first, tall - 1)
            other = jnp.minimum(s + (1 - half) * first, tall - 1)
            for o in range(rows):
                given[c][s, o] = risen[c][o, other]
                kept[c][s, o] = risen[c][o, mine]
            return carry
        lax.fori_loop(0, cap, settle, 0)
        give = pltpu.make_async_remote_copy(
            src_ref=given[c], dst_ref=final[c].at[half],
            send_sem=give_send.at[c], recv_sem=give_recv.at[c], device_id=mate, device_id_type=MESH)
        give.start()
        keep = pltpu.make_async_copy(kept[c], final[c].at[half], keep_sem.at[c])
        keep.start()
        gives.append((give, keep))

    if not relay:
        row_copies = []
        for c in range(chunks):
            for copy in pair_copies[c]:
                copy.wait_recv()
            sent = []
            for o in list(range(rows - 1, 0, -1)) + [0]:
                row = lax.rem(z + o, rows)

                def lift(k, carry, o=o, c=c, row=row):
                    tile = landed[c][row_list[row * tall + k]]
                    if o > 0:
                        lifted[c][o - 1, k] = tile
                    else:
                        risen[c][0, k] = tile
                    return carry
                lax.fori_loop(0, tall, lift, 0, unroll=4)
                if o > 0:
                    copy = pltpu.make_async_remote_copy(
                        src_ref=lifted[c].at[o - 1], dst_ref=risen[c].at[o],
                        send_sem=row_send.at[c, o - 1], recv_sem=row_recv.at[c, o - 1],
                        device_id=along(o), device_id_type=MESH)
                    copy.start()
                    sent.append(copy)
            row_copies.append(sent)
            unsent.extend(sent)
        for c in range(chunks):
            for copy in row_copies[c]:
                copy.wait_recv()
            settle_all(c)
    else:
        pooled, crossed, passed = groups[7:10]
        far_list, far_send, far_recv, pass_send, pass_recv = sems[10:]
        near, far_in, far_out = (origin_of(z, rows, k) for k in (1, 2, 3))
        inner = jnp.logical_or(z == 1, z == 2)
        outer = jnp.logical_not(inner)
        role = jnp.where(inner, 0, 1)
        lead = tallies[far_in] + tallies[rows + far_in]
        skip = tallies[z] + tallies[rows + z]

        def gather_far(k, carry):
            at = jnp.where(k < lead, far_in * tall + k, far_out * tall + k - lead)
            far_list[k] = row_list[jnp.minimum(at, rows * tall - 1)]
            return carry
        lax.fori_loop(0, far, gather_far, 0, unroll=4)

        near_copies = {}

        def far_copy(c, place):
            return pltpu.make_async_remote_copy(
                src_ref=pooled[c], dst_ref=crossed[c].at[place],
                send_sem=far_send.at[c], recv_sem=far_recv.at[c, place],
                device_id=(gx, far_in), device_id_type=MESH)

        def pass_copy(c, place):
            return pltpu.make_async_remote_copy(
                src_ref=passed[c].at[place], dst_ref=risen[c].at[2 + place, pl.ds(0, end)],
                send_sem=pass_send.at[c, place], recv_sem=pass_recv.at[c, place],
                device_id=(gx, near), device_id_type=MESH)

        def send_rows(c):
            for copy in pair_copies[c]:
                copy.wait_recv()

            def pool(k, carry):
                pooled[c][k] = landed[c][far_list[k]]
                return carry
            lax.fori_loop(0, far, pool, 0, unroll=4)
            copy = far_copy(c, role)
            copy.start()
            unsent.append(copy)

            def lift(k, carry):
                lifted[c][k] = landed[c][row_list[near * tall + k]]
                return carry
            lax.fori_loop(0, tall, lift, 0, unroll=4)
            copy = pltpu.make_async_remote_copy(
                src_ref=lifted[c], dst_ref=risen[c].at[1],
                send_sem=row_send.at[c], recv_sem=row_recv.at[c],
                device_id=(gx, near), device_id_type=MESH)
            copy.start()
            unsent.append(copy)
            near_copies[c] = copy

            def own(k, carry):
                risen[c][0, k] = landed[c][row_list[z * tall + k]]
                return carry
            lax.fori_loop(0, tall, own, 0, unroll=4)

        def hand_on(c):
            @pl.when(inner)
            def _():
                for place in range(2):
                    far_copy(c, place).wait_recv()
                for place in range(2):
                    def onward(k, carry, place=place):
                        passed[c][place, k] = crossed[c][place, jnp.minimum(skip + k, far - 1)]
                        return carry
                    lax.fori_loop(0, end, onward, 0, unroll=4)
                    pass_copy(c, place).start()

                    def land(k, carry, place=place):
                        risen[c][2 + place, k] = crossed[c][place, k]
                        return carry
                    lax.fori_loop(0, tall, land, 0, unroll=4)

        def close(c):
            near_copies[c].wait_recv()

            @pl.when(outer)
            def _():
                for place in range(2):
                    pass_copy(c, place).wait_recv()
            settle_all(c)

        pace = far / wide
        events = []
        for c in range(chunks):
            begin, close_at = starts[c]
            if c not in early:
                events.append((float(begin - ahead), -1, c, pack_chunk))
            events.append((float(close_at), 0, c, send_rows))
            events.append((starts[0][1] + pace * close_at, 1, c, hand_on))
            events.append((starts[0][1] + pace * (2 * close_at - begin), 2, c, close))
        for _, _, c, act in sorted(events, key=lambda e: (e[0], e[1], e[2])):
            act(c)

        @pl.when(inner)
        def _():
            for c in range(chunks):
                for place in range(2):
                    pass_copy(c, place).wait_send()

    for copy in unsent:
        copy.wait_send()
    for give, keep in gives:
        give.wait()
        keep.wait()


def finish(rows, chunks, tally, *refs):
    final, regional = refs[:-1], refs[-1]
    z = lax.axis_index("gy")
    slot = pl.program_id(0)
    side = regional.shape[3]
    times = regional.shape[0] // rows
    place = {unit: (c, i) for c, chunk in enumerate(chunks) for i, unit in enumerate(chunk)}

    @pl.when(slot < tally[0])
    def _():
        for h in range(2):
            for r in range(side // (2 * PART)):
                span = pl.ds(h * (side // 2) + r * PART, PART)
                tiles = {}
                for t in range(times):
                    c, i = place[(r, t)]
                    for o in range(rows):
                        tiles[o, t] = final[c][h, 0, o, i]
                mean = sum(tiles.values()) * jnp.float32(1.0 / (rows * times))
                for o in range(rows):
                    start = origin_of(z, rows, o) * times
                    for t in range(times):
                        regional[start + t, 0, 0, span, :] = tiles[o, t] - mean

    @pl.when(slot >= tally[0])
    def _():
        regional[...] = jnp.zeros_like(regional)


def levels(most, steps):
    return sorted({-(-most * s // 48) for s in steps})


def on_device(field, zone, slot, spins, tally):
    times, per_group, side, _ = field.shape
    columns = lax.axis_size("gx")
    rows = lax.axis_size("gy")
    pairs = columns // 2
    cap = 2 * per_group // rows
    per_pair = 4 * (2 * per_group // columns)
    per_row = 2 * cap
    chunks = chunk_units(times, side)
    tiles = [(len(chunk), PART, side) for chunk in chunks]
    ends = [sum(len(chunk) for chunk in chunks[:c + 1]) for c in range(len(chunks))]
    starts = tuple((end - tile[0], end) for end, tile in zip(ends, tiles))
    smem = pl.BlockSpec(memory_space=pltpu.SMEM)
    anywhere = pl.BlockSpec(memory_space=pl.ANY)
    i32 = jnp.int32
    relay = rows == 4
    narrow = levels(per_pair, (40,))[0]
    if relay:
        ends = levels(per_row, (40, 48))
        sizes = [(narrow, per_row, far, end) for far in levels(2 * per_row, (32, 34, 36)) for end in ends]
        sizes += [(narrow, per_row, far, per_row) for far in levels(2 * per_row, (40,))]
    else:
        sizes = [(narrow, tall, 2 * per_row, tall) for tall in levels(per_row, (36, 42))]
    sizes.append((per_pair, per_row, 2 * per_row, per_row))
    *turned, send_table, pick_table, tallies, choice = pl.pallas_call(
        functools.partial(prepare, (pairs, rows, per_group, per_pair, cap, chunks, sizes)),
        grid=(per_group // STEP_BLOCKS,),
        in_specs=[smem, smem, smem, pl.BlockSpec((times, STEP_BLOCKS, side, side), lambda i: (0, i, 0, 0))],
        out_specs=[
            *[pl.BlockSpec((2, STEP_BLOCKS) + tile, lambda i: (0, i, 0, 0, 0)) for tile in tiles],
            smem, smem, smem, smem,
        ],
        out_shape=[
            *[jax.ShapeDtypeStruct((2, per_group) + tile, jnp.float32) for tile in tiles],
            jax.ShapeDtypeStruct((pairs * per_pair + 1,), i32),
            jax.ShapeDtypeStruct((per_row * rows + 1,), i32),
            jax.ShapeDtypeStruct((2 * rows,), i32),
            jax.ShapeDtypeStruct((1,), i32),
        ],
        scratch_shapes=[pltpu.SMEM((columns * rows,), i32), pltpu.SMEM((pairs * pairs,), i32)],
        name="prepare",
    )(zone, slot, spins, field)

    def moved(wide, tall, far, end, tag):
        def vmem(*lead):
            return [pltpu.VMEM(lead + tile, jnp.float32) for tile in tiles]
        dma = pltpu.SemaphoreType.DMA
        count = len(chunks)
        along = (count,) if relay else (count, rows - 1)
        buffers = [
            *vmem(2 * per_group),
            *vmem(pairs - 1, wide),
            *vmem(pairs * per_pair),
            *(vmem(tall) if relay else vmem(rows - 1, tall)),
            *vmem(rows, tall),
            *vmem(cap, rows),
            *vmem(cap, rows),
            *(vmem(far) + vmem(2, far) + vmem(2, end) if relay else []),
            pltpu.SMEM((rows * tall,), i32),
            dma((count,)), dma((count,)), dma((count,)),
            dma((count, pairs - 1)), dma((count, pairs - 1)),
            dma(along), dma(along),
            dma((count,)), dma((count,)), dma((count,)),
        ]
        if relay:
            buffers += [pltpu.SMEM((far,), i32), dma((count,)), dma((count, 2)), dma((count, 2)), dma((count, 2))]
        return lambda: pl.pallas_call(
            functools.partial(exchange, (pairs, rows, per_group, per_pair, wide, tall, far, end, cap, starts)),
            in_specs=[smem, smem, smem] + [anywhere] * count,
            out_specs=[anywhere] * count,
            out_shape=[jax.ShapeDtypeStruct((2, cap, rows) + tile, jnp.float32) for tile in tiles],
            scratch_shapes=buffers,
            compiler_params=pltpu.CompilerParams(collective_id=tag, has_side_effects=True, vmem_limit_bytes=60 * 2**20),
            name=f"exchange_{tag}",
        )(send_table, pick_table, tallies, *turned)

    final = lax.switch(choice[0], [moved(*size, tag) for tag, size in enumerate(sizes)])

    return pl.pallas_call(
        functools.partial(finish, rows, chunks),
        grid_spec=pltpu.PrefetchScalarGridSpec(
            num_scalar_prefetch=1,
            grid=(cap,),
            in_specs=[pl.BlockSpec(
                (2, 1, rows) + tile,
                lambda s, count: (0, jnp.maximum(jnp.minimum(s, count[0] - 1), 0), 0, 0, 0, 0)) for tile in tiles],
            out_specs=pl.BlockSpec((rows * times, 1, 1, side, side), lambda s, count: (0, 0, s, 0, 0)),
        ),
        out_shape=jax.ShapeDtypeStruct((rows * times, 1, cap, side, side), jnp.float32),
        name="finish",
    )(tally, *final)


def solution(mesh):
    placed = (P("gy", "gx", None, None), P(), P(), P(), P(("gx", "gy")))
    return jax.shard_map(
        on_device,
        mesh=mesh,
        in_specs=placed,
        out_specs=P(None, ("gx", "gy"), None, None, None),
        check_vma=False,
    )
```
